64 devices in a mesh: rep: 4 (over x, y), dp: 16 (over z, core).
Axes of the slice: x: 2, y: 2, z: 8, core: 2. Of those that a mesh axis runs over, the one named last changes fastest.
The devices are a block of a 4x4x8 slice.
Arguments:
- a: bfloat16 [64, 4, 4096, 896], P(('rep', 'dp')), parts along dimension 0
- g: bfloat16 [64, 4, 4096, 2304], P(('rep', 'dp')), parts along dimension 0
Outputs:
- output: bfloat16 [16, 896, 2304], P('rep'), parts along dimension 0
There are 4 independent parts. The reference program is written for one: setup_inputs(seed, part) draws one part's arguments, and reference() takes and returns one part's arrays. A program takes and returns all parts, laid end to end along the dimension named above; each array names one.
All inputs are finite; a program needn't handle non-finite values.
Results may differ from the reference program's by a relative error of at most 0.012.
Values are sent between devices in bfloat16 or wider.
A program may use at most 768 MiB of HBM per device.

```python
import jax
import jax.numpy as jnp
from jax import lax

DEVICES = 16
MATRICES = 4
TOKENS = 4096
D = 896
FF = 2304


def setup_inputs(seed: int = 0, part: int = 0) -> dict:
    ka, kg, ks = (jax.random.fold_in(k, part) for k in jax.random.split(jax.random.key(seed), 3))
    size = 2.0 ** jax.random.uniform(ks, (DEVICES, MATRICES, 1, 1), jnp.float32, -1.0, 1.0)
    a = jax.random.normal(ka, (DEVICES, MATRICES, TOKENS, D), jnp.float32)
    g = size * jax.random.normal(kg, (DEVICES, MATRICES, TOKENS, FF), jnp.float32) * (DEVICES * TOKENS) ** -0.5
    return {"a": a.astype(jnp.bfloat16), "g": g.astype(jnp.bfloat16)}


def reference(a, g):
    def take(so_far, one):
        return so_far + jnp.einsum("ntd,ntf->ndf", *one, preferred_element_type=jnp.float32), None

    return lax.scan(take, jnp.zeros((MATRICES, D, FF), jnp.float32), (a, g))[0].astype(jnp.bfloat16)
```

```python
import functools

import jax
import jax.numpy as jnp
from jax import lax
from jax.experimental import pallas as pl
from jax.experimental.pallas import tpu as pltpu
from jax.sharding import PartitionSpec as P

WIDTH = 256
LAG = 3
SLOTS = 4
MESH = pl.DeviceIdType.MESH


def kernel(
    chips, a, g, total,
    a_buf, g_buf, term, x_out, x_in,
    a_sem, g_sem, xs_sem, xr_sem, rs_send, rs_recv, ag_send, ag_recv, d2_send, d2_recv, free_sem,
):
    n_mat, ff = g.shape[1], g.shape[3]
    d_rows = a.shape[3]
    half = d_rows // 2
    cols = ff // WIDTH
    tiles = n_mat * cols // 2
    me = lax.axis_index("dp")
    z, core = me // 2, lax.rem(me, 2)
    partner = {"dp": z * 2 + 1 - core}

    def ring(d):
        place = jnp.where(d == 0, z, chips - 1 - z)
        to = lax.rem(z + jnp.where(d == 0, 1, chips - 1), chips)
        return place, {"dp": to * 2 + core}

    def start_of(b):
        return tiles * b // chips

    def tile_of(d, q):
        place, _ = ring(d)
        u = lax.rem(start_of(place) + 2 * tiles - 1 - q, tiles)
        return d * tiles + u

    def size_of(b):
        return start_of(b + 1) - start_of(b)

    def place_of(t):
        return t // cols, pl.ds(pl.multiple_of(lax.rem(t, cols) * WIDTH, WIDTH), WIDTH)

    def a_copy(n):
        return pltpu.make_async_copy(a.at[0, n], a_buf.at[n], a_sem.at[n])

    def g_copy(d, q):
        n, c = place_of(tile_of(d, q))
        slot = lax.rem(q, 2)
        return pltpu.make_async_copy(g.at[0, n, :, c], g_buf.at[d, slot], g_sem.at[d, slot])

    def x_copy(t):
        slot = lax.rem(t, SLOTS)
        return pltpu.make_async_remote_copy(
            src_ref=x_out.at[slot], dst_ref=x_in.at[slot], send_sem=xs_sem.at[slot], recv_sem=xr_sem.at[slot],
            device_id=partner, device_id_type=MESH)

    def move(t, to, send, recv):
        return pltpu.make_async_remote_copy(
            src_ref=total.at[t, core], dst_ref=total.at[t, core], send_sem=send.at[t], recv_sem=recv.at[t],
            device_id=to, device_id_type=MESH)

    def from_partner(t):
        return pltpu.make_async_remote_copy(
            src_ref=total.at[t, 1 - core], dst_ref=total.at[t, 1 - core], send_sem=d2_send.at[t], recv_sem=d2_recv.at[t],
            device_id=partner, device_id_type=MESH)

    def give(d, q):
        move(tile_of(d, q), ring(d)[1], rs_send, rs_recv).wait_send()
        pl.semaphore_signal(free_sem.at[d], inc=1, device_id=ring(1 - d)[1], device_id_type=MESH)

    first = [tile_of(d, 0) // cols for d in range(2)]
    other = [4 * d + 1 - first[d] for d in range(2)]
    for d in range(2):
        g_copy(d, 0).start()
        a_copy(first[d]).start()
    for d in range(2):
        g_copy(d, 1).start()
    for d in range(2):
        a_copy(other[d]).start()

    barrier = pltpu.get_barrier_semaphore()
    for to in (ring(0)[1], ring(1)[1], partner):
        pl.semaphore_signal(barrier, inc=1, device_id=to, device_id_type=MESH)
    pl.semaphore_wait(barrier, 3)

    def compute(d, q):
        t = tile_of(d, q)
        n = t // cols
        slot = lax.rem(q, 2)
        x_slot = lax.rem(2 * q + d, SLOTS)
        g_copy(d, q).wait()
        start = tile_of(d, 0)

        @pl.when(q == 0)
        def _():
            a_copy(start // cols).wait()

        @pl.when(q == lax.rem(start, cols) + 1)
        def _():
            a_copy(4 * d + 1 - start // cols).wait()

        product = lax.dot_general(
            a_buf[n], g_buf[d, slot], (((0,), (0,)), ((), ())), preferred_element_type=jnp.float32)
        term[d, 0] = product[:half]
        term[d, 1] = product[half:]
        x_out[x_slot] = term[d, 1 - core].astype(jnp.bfloat16)
        x_copy(2 * q + d).start()

        @pl.when(q + 2 < tiles)
        def _():
            g_copy(d, q + 2).start()

    def reduce(d, q):
        place, to = ring(d)
        t = tile_of(d, q)
        before = lax.rem(place + chips - 1, chips)
        x_copy(2 * q + d).wait()
        term[d, core] += x_in[lax.rem(2 * q + d, SLOTS)].astype(jnp.float32)

        @pl.when(q >= size_of(before))
        def _():
            move(t, to, rs_send, rs_recv).wait_recv()
            term[d, core] += total[t, core].astype(jnp.float32)

        total[t, core] = term[d, core].astype(jnp.bfloat16)
        last = q >= tiles - size_of(place)

        @pl.when(jnp.logical_not(last))
        def _():
            move(t, to, rs_send, rs_recv).start()

        @pl.when(jnp.logical_and(q >= LAG, q - LAG < tiles - size_of(place)))
        def _():
            give(d, q - LAG)

        @pl.when(last)
        def _():
            pl.semaphore_wait(free_sem.at[d], 1)
            move(t, to, ag_send, ag_recv).start()
            move(t, partner, d2_send, d2_recv).start()

    def step(t, _):
        compute(lax.rem(t, 2), t // 2)

        @pl.when(t > 0)
        def _():
            reduce(lax.rem(t - 1, 2), (t - 1) // 2)

        return 0

    lax.fori_loop(0, 2 * tiles, step, 0)
    reduce(1, tiles - 1)

    for d in range(2):
        for i in range(LAG):
            @pl.when(tiles - LAG + i < tiles - size_of(ring(d)[0]))
            def _():
                give(d, tiles - LAG + i)

    def gather(r, _):
        for d in range(2):
            place, to = ring(d)
            after = lax.rem(place + 1, chips)
            count = tiles - size_of(place)
            t = tile_of(d, r)

            @pl.when(r < count)
            def _():
                move(t, to, ag_send, ag_recv).wait_recv()

                @pl.when(r < count - size_of(after))
                def _():
                    pl.semaphore_wait(free_sem.at[d], 1)
                    move(t, to, ag_send, ag_recv).start()

                move(t, partner, d2_send, d2_recv).start()

        for d in range(2):
            from_partner(tile_of(d, r + tiles - 1)).wait_recv()
        return 0

    lax.fori_loop(0, tiles, gather, 0)

    def drain(q, _):
        for d in range(2):
            place, to = ring(d)
            after = lax.rem(place + 1, chips)
            count = tiles - size_of(place)
            t = tile_of(d, q)
            move(t, partner, d2_send, d2_recv).wait_send()

            @pl.when(jnp.logical_or(q < count - size_of(after), q >= count))
            def _():
                move(t, to, ag_send, ag_recv).wait_send()
        return 0

    lax.fori_loop(0, tiles, drain, 0)


def writer(sums, out, sem):
    tiles, _, half, _ = sums.shape
    cols = tiles // out.shape[0]

    def write(i, _):
        t, h = i // 2, lax.rem(i, 2)
        rows = pl.ds(pl.multiple_of(h * half, 8), half)
        columns = pl.ds(pl.multiple_of(lax.rem(t, cols) * WIDTH, WIDTH), WIDTH)
        pltpu.make_async_copy(sums.at[t, h], out.at[t // cols, rows, columns], sem).start()
        return 0

    lax.fori_loop(0, 2 * tiles, write, 0)
    pltpu.make_async_copy(out, out, sem).wait()


def sums(chips, a, g):
    _, n_mat, tokens, d_rows = a.shape
    ff = g.shape[-1]
    half = d_rows // 2
    tiles = n_mat * (ff // WIDTH)
    dma = pltpu.SemaphoreType.DMA
    total = pl.pallas_call(
        functools.partial(kernel, chips),
        out_shape=pltpu.VMEM((tiles, 2, half, WIDTH), jnp.bfloat16),
        in_specs=[pl.BlockSpec(memory_space=pl.ANY)] * 2,
        out_specs=pl.BlockSpec(memory_space=pltpu.VMEM),
        scratch_shapes=[
            pltpu.VMEM((n_mat, tokens, d_rows), jnp.bfloat16),
            pltpu.VMEM((2, 2, tokens, WIDTH), jnp.bfloat16),
            pltpu.VMEM((2, 2, half, WIDTH), jnp.float32),
            pltpu.VMEM((SLOTS, half, WIDTH), jnp.bfloat16),
            pltpu.VMEM((SLOTS, half, WIDTH), jnp.bfloat16),
            dma((n_mat,)), dma((2, 2)), dma((SLOTS,)), dma((SLOTS,)),
            dma((tiles,)), dma((tiles,)), dma((tiles,)), dma((tiles,)), dma((tiles,)), dma((tiles,)),
            pltpu.SemaphoreType.REGULAR((2,)),
        ],
        compiler_params=pltpu.CompilerParams(
            collective_id=0, has_side_effects=True, vmem_limit_bytes=46 << 20),
        name="sums",
    )(a, g)
    return pl.pallas_call(
        writer,
        out_shape=jax.ShapeDtypeStruct((n_mat, d_rows, ff), jnp.bfloat16),
        in_specs=[pl.BlockSpec(memory_space=pltpu.VMEM)],
        out_specs=pl.BlockSpec(memory_space=pl.ANY),
        scratch_shapes=[dma(())],
        compiler_params=pltpu.CompilerParams(vmem_limit_bytes=40 << 20),
        name="writer",
    )(pltpu.with_memory_space_constraint(total, pltpu.VMEM))


def solution(mesh):
    chips = mesh.shape["dp"] // 2
    return jax.shard_map(
        functools.partial(sums, chips), mesh=mesh,
        in_specs=(P(("rep", "dp")), P(("rep", "dp"))), out_specs=P("rep"), check_vma=False)
```

```python
import functools

import jax
import jax.numpy as jnp
from jax import lax
from jax.experimental import pallas as pl
from jax.experimental.pallas import tpu as pltpu
from jax.sharding import PartitionSpec as P

WIDTH = 256
LAG = 3
SLOTS = 4
MESH = pl.DeviceIdType.MESH


def kernel(
    chips, a, g, total,
    a_buf, g_buf, term, x_out, x_in,
    a_sem, g_sem, xs_sem, xr_sem, rs_send, ag_send, recv, swap_sem, free_sem,
):
    n_mat, ff = g.shape[1], g.shape[3]
    d_rows = a.shape[3]
    half = d_rows // 2
    cols = ff // WIDTH
    tiles = n_mat * cols // 2
    me = lax.axis_index("dp")
    z, core = me // 2, lax.rem(me, 2)
    partner = {"dp": z * 2 + 1 - core}

    def ring(d):
        place = jnp.where(d == 0, z, chips - 1 - z)
        to = lax.rem(z + jnp.where(d == 0, 1, chips - 1), chips)
        return place, {"dp": to * 2 + core}

    def start_of(b):
        return tiles * b // chips

    def tile_of(d, q):
        place, _ = ring(d)
        u = lax.rem(start_of(place) + 2 * tiles - 1 - q, tiles)
        return d * tiles + u

    def size_of(b):
        return start_of(b + 1) - start_of(b)

    def place_of(t):
        return t // cols, pl.ds(pl.multiple_of(lax.rem(t, cols) * WIDTH, WIDTH), WIDTH)

    def a_copy(n):
        return pltpu.make_async_copy(a.at[0, n], a_buf.at[n], a_sem.at[n])

    def g_copy(d, q):
        n, c = place_of(tile_of(d, q))
        slot = lax.rem(q, 2)
        return pltpu.make_async_copy(g.at[0, n, :, c], g_buf.at[d, slot], g_sem.at[d, slot])

    def x_copy(t):
        slot = lax.rem(t, SLOTS)
        return pltpu.make_async_remote_copy(
            src_ref=x_out.at[slot], dst_ref=x_in.at[slot], send_sem=xs_sem.at[slot], recv_sem=xr_sem.at[slot],
            device_id=partner, device_id_type=MESH)

    def move(t, to, send):
        return pltpu.make_async_remote_copy(
            src_ref=total.at[t, core], dst_ref=total.at[t, core], send_sem=send, recv_sem=recv.at[t],
            device_id=to, device_id_type=MESH)

    def running(d, q):
        return move(tile_of(d, q), ring(d)[1], rs_send.at[d, lax.rem(q, LAG + 1)])

    def final(d, t, s):
        return move(t, ring(d)[1], ag_send.at[d, lax.rem(s, LAG + 1)])

    def swap(t):
        return pltpu.make_async_remote_copy(
            src_ref=total.at[t, core], dst_ref=total.at[t, core], send_sem=swap_sem.at[0], recv_sem=swap_sem.at[1],
            device_id=partner, device_id_type=MESH)

    def give(d, q):
        running(d, q).wait_send()
        pl.semaphore_signal(free_sem.at[d], inc=1, device_id=ring(1 - d)[1], device_id_type=MESH)

    g_copy(0, 0).start()
    a_copy(tile_of(0, 0) // cols).start()

    barrier = pltpu.get_barrier_semaphore()
    for to in (ring(0)[1], ring(1)[1], partner):
        pl.semaphore_signal(barrier, inc=1, device_id=to, device_id_type=MESH)
    pl.semaphore_wait(barrier, 3)

    g_copy(1, 0).start()
    a_copy(tile_of(1, 0) // cols).start()
    for d in range(2):
        g_copy(d, 1).start()

    def compute(d, q):
        t = tile_of(d, q)
        n = t // cols
        slot = lax.rem(q, 2)
        x_slot = lax.rem(2 * q + d, SLOTS)
        g_copy(d, q).wait()
        start = tile_of(d, 0)

        @pl.when(q == 0)
        def _():
            a_copy(start // cols).wait()
            a_copy(4 * d + 1 - start // cols).start()

        @pl.when(q == lax.rem(start, cols) + 1)
        def _():
            a_copy(4 * d + 1 - start // cols).wait()

        product = lax.dot_general(
            a_buf[n], g_buf[d, slot], (((0,), (0,)), ((), ())), preferred_element_type=jnp.float32)
        low, high = product[:half], product[half:]
        x_out[x_slot] = jnp.where(core == 0, high, low).astype(jnp.bfloat16)
        term[d] = jnp.where(core == 0, low, high)
        x_copy(2 * q + d).start()

        @pl.when(q + 2 < tiles)
        def _():
            g_copy(d, q + 2).start()

    def reduce(d, q):
        place, _ = ring(d)
        t = tile_of(d, q)
        before = lax.rem(place + chips - 1, chips)
        sent = tiles - size_of(place)
        x_copy(2 * q + d).wait()

        @pl.when(q < size_of(before))
        def _():
            total[t, core] = (term[d] + x_in[lax.rem(2 * q + d, SLOTS)].astype(jnp.float32)).astype(jnp.bfloat16)

        @pl.when(q >= size_of(before))
        def _():
            running(d, q).wait_recv()
            here = term[d] + x_in[lax.rem(2 * q + d, SLOTS)].astype(jnp.float32)
            total[t, core] = (here + total[t, core].astype(jnp.float32)).astype(jnp.bfloat16)

        @pl.when(q < sent)
        def _():
            running(d, q).start()

        @pl.when(jnp.logical_and(q >= LAG, q - LAG < sent))
        def _():
            give(d, q - LAG)

        @pl.when(q >= sent)
        def _():
            pl.semaphore_wait(free_sem.at[d], 1)
            final(d, t, q - sent).start()
            swap(t).start()

    def step(t, _):
        compute(lax.rem(t, 2), t // 2)

        @pl.when(t > 0)
        def _():
            reduce(lax.rem(t - 1, 2), (t - 1) // 2)

        return 0

    lax.fori_loop(0, 2 * tiles, step, 0)
    reduce(1, tiles - 1)

    for d in range(2):
        for i in range(LAG):
            @pl.when(tiles - LAG + i < tiles - size_of(ring(d)[0]))
            def _():
                give(d, tiles - LAG + i)

    def gather(r, _):
        for d in range(2):
            place, _ = ring(d)
            count = tiles - size_of(place)
            t = tile_of(d, r)
            s = size_of(place) + r

            @pl.when(r < count)
            def _():
                final(d, t, s).wait_recv()

                @pl.when(r < count - size_of(lax.rem(place + 1, chips)))
                def _():
                    @pl.when(s > LAG)
                    def _():
                        final(d, t, s).wait_send()

                    pl.semaphore_wait(free_sem.at[d], 1)
                    final(d, t, s).start()

                swap(t).start()

        return 0

    lax.fori_loop(0, tiles, gather, 0)

    for d in range(2):
        for i in range(LAG + 1):
            final(d, 0, i).wait_send()
    swap(slice(None)).wait()


def writer(sums, out, sem):
    tiles, _, half, _ = sums.shape
    cols = tiles // out.shape[0]

    def write(i, _):
        t, h = i // 2, lax.rem(i, 2)
        rows = pl.ds(pl.multiple_of(h * half, 8), half)
        columns = pl.ds(pl.multiple_of(lax.rem(t, cols) * WIDTH, WIDTH), WIDTH)
        pltpu.make_async_copy(sums.at[t, h], out.at[t // cols, rows, columns], sem).start()
        return 0

    lax.fori_loop(0, 2 * tiles, write, 0)
    pltpu.make_async_copy(out, out, sem).wait()


def sums(chips, a, g):
    _, n_mat, tokens, d_rows = a.shape
    ff = g.shape[-1]
    half = d_rows // 2
    tiles = n_mat * (ff // WIDTH)
    dma = pltpu.SemaphoreType.DMA
    total = pl.pallas_call(
        functools.partial(kernel, chips),
        out_shape=pltpu.VMEM((tiles, 2, half, WIDTH), jnp.bfloat16),
        in_specs=[pl.BlockSpec(memory_space=pl.ANY)] * 2,
        out_specs=pl.BlockSpec(memory_space=pltpu.VMEM),
        scratch_shapes=[
            pltpu.VMEM((n_mat, tokens, d_rows), jnp.bfloat16),
            pltpu.VMEM((2, 2, tokens, WIDTH), jnp.bfloat16),
            pltpu.VMEM((2, half, WIDTH), jnp.float32),
            pltpu.VMEM((SLOTS, half, WIDTH), jnp.bfloat16),
            pltpu.VMEM((SLOTS, half, WIDTH), jnp.bfloat16),
            dma((n_mat,)), dma((2, 2)), dma((SLOTS,)), dma((SLOTS,)),
            dma((2, LAG + 1)), dma((2, LAG + 1)), dma((tiles,)), dma((2,)),
            pltpu.SemaphoreType.REGULAR((2,)),
        ],
        compiler_params=pltpu.CompilerParams(
            collective_id=0, has_side_effects=True, vmem_limit_bytes=46 << 20),
        name="sums",
    )(a, g)
    return pl.pallas_call(
        writer,
        out_shape=jax.ShapeDtypeStruct((n_mat, d_rows, ff), jnp.bfloat16),
        in_specs=[pl.BlockSpec(memory_space=pltpu.VMEM)],
        out_specs=pl.BlockSpec(memory_space=pl.ANY),
        scratch_shapes=[dma(())],
        compiler_params=pltpu.CompilerParams(vmem_limit_bytes=40 << 20),
        name="writer",
    )(pltpu.with_memory_space_constraint(total, pltpu.VMEM))


def solution(mesh):
    chips = mesh.shape["dp"] // 2
    return jax.shard_map(
        functools.partial(sums, chips), mesh=mesh,
        in_specs=(P(("rep", "dp")), P(("rep", "dp"))), out_specs=P("rep"), check_vma=False)
```
